32 devices in a mesh: dp: 2 (over x), tp: 16 (over y, z, core).
Axes of the slice: x: 2, y: 2, z: 4, core: 2. Of those that a mesh axis runs over, the one named last changes fastest.
Arguments:
- x: bfloat16 [128, 8192], P('dp'), parts along dimension 0
- k_cache: bfloat16 [128, 1024, 64, 128], P('dp', None, 'tp'), parts along dimension 0
- v_cache: bfloat16 [128, 1024, 64, 128], P('dp', None, 'tp'), parts along dimension 0
- gain_a: bfloat16 [8192], replicated
- wq: bfloat16 [8192, 8192], P(None, 'tp')
- wo: bfloat16 [8192, 8192], P('tp')
- gain_m: bfloat16 [8192], replicated
- w_gate: bfloat16 [8192, 24576], P(None, 'tp')
- w_up: bfloat16 [8192, 24576], P(None, 'tp')
- w_down: bfloat16 [24576, 8192], P('tp')
Outputs:
- output: bfloat16 [128, 8192], P('dp'), parts along dimension 0
There are 2 independent parts. The reference program is written for one: setup_inputs(seed, part) draws one part's arguments, and reference() takes and returns one part's arrays. A program takes and returns all parts, laid end to end along the dimension named above; an argument that names none is the same for every part.
All inputs are finite; a program needn't handle non-finite values.
Results may differ from the reference program's by a relative error of at most 0.017.
Values are sent between devices in bfloat16 or wider.
A program may use at most 2 GiB of HBM per device.

```python
import jax
import jax.numpy as jnp
from jax import lax

BATCH = 64
CACHE = 1024
D = 8192
HEADS = 64
KV_HEADS = 64
HEAD = 128
FF = 24576
THETA = 10000


def setup_inputs(seed: int = 0, part: int = 0) -> dict:
    kx, kc, kw, kn, kq, ko, km, kg, ku, kd = jax.random.split(jax.random.key(seed), 10)
    kx, kc, kw = (jax.random.fold_in(k, part) for k in (kx, kc, kw))

    def weights(key, rows, columns):
        return jax.random.normal(key, (rows, columns), jnp.float32) * rows**-0.5

    drawn = {
        "x": jax.random.normal(kx, (BATCH, D), jnp.float32),
        "k_cache": 2 * jax.random.normal(kc, (BATCH, CACHE, KV_HEADS, HEAD), jnp.float32),
        "v_cache": 4 * jax.random.normal(kw, (BATCH, CACHE, KV_HEADS, HEAD), jnp.float32),
        "gain_a": 1 + 0.1 * jax.random.normal(kn, (D,), jnp.float32),
        "wq": 2 * weights(kq, D, HEADS * HEAD),
        "wo": weights(ko, HEADS * HEAD, D),
        "gain_m": 1 + 0.1 * jax.random.normal(km, (D,), jnp.float32),
        "w_gate": weights(kg, D, FF),
        "w_up": weights(ku, D, FF),
        "w_down": 2 * weights(kd, FF, D),
    }
    return {k: v.astype(jnp.bfloat16) for k, v in drawn.items()}


def normed(x, gain):
    wide = x.astype(jnp.float32)
    scale = lax.rsqrt(jnp.mean(wide * wide, -1, keepdims=True) + 1e-6)
    return (wide * scale * gain.astype(jnp.float32)).astype(jnp.bfloat16)


def turned(t, place, theta):
    half = t.shape[-1] // 2
    angle = place.astype(jnp.float32)[:, None] * theta ** (-jnp.arange(half, dtype=jnp.float32) / half)
    cos, sin = jnp.cos(angle)[:, None], jnp.sin(angle)[:, None]
    a, b = t[..., :half].astype(jnp.float32), t[..., half:].astype(jnp.float32)
    return jnp.concatenate([a * cos - b * sin, b * cos + a * sin], -1).astype(jnp.bfloat16)


def matmul(a, w):
    return jnp.dot(a, w, preferred_element_type=jnp.float32).astype(jnp.bfloat16)


def einsum(form, a, b):
    return jnp.einsum(form, a.astype(jnp.float32), b.astype(jnp.float32))


def seen_by(a, wq, k_cache, v_cache, head, theta):
    batch, cache, kv_heads = k_cache.shape[:3]
    place = jnp.full((batch,), cache - 1)
    q = turned(matmul(a, wq).reshape(batch, -1, head), place, theta).reshape(batch, kv_heads, -1, head)
    scores = einsum("bgsd,bugd->bgsu", q, k_cache) * head**-0.5
    weights = jax.nn.softmax(scores, -1).astype(jnp.bfloat16)
    return einsum("bgsu,bugd->bgsd", weights, v_cache).astype(jnp.bfloat16).reshape(batch, -1)


def hidden_of(b, w_gate, w_up):
    gate = jnp.dot(b, w_gate, preferred_element_type=jnp.float32)
    up = jnp.dot(b, w_up, preferred_element_type=jnp.float32)
    return (jax.nn.silu(gate) * up).astype(jnp.bfloat16)


def reference(x, k_cache, v_cache, gain_a, wq, wo, gain_m, w_gate, w_up, w_down):
    seen = seen_by(normed(x, gain_a), wq, k_cache, v_cache, HEAD, THETA)
    h = (x.astype(jnp.float32) + jnp.dot(seen, wo, preferred_element_type=jnp.float32)).astype(jnp.bfloat16)
    hidden = hidden_of(normed(h, gain_m), w_gate, w_up)
    return (h.astype(jnp.float32) + jnp.dot(hidden, w_down, preferred_element_type=jnp.float32)).astype(jnp.bfloat16)
```

```python
import jax
import jax.numpy as jnp
from jax import lax
from jax.experimental import pallas as pl
from jax.experimental.pallas import tpu as pltpu
from jax.sharding import PartitionSpec as P

HEAD = 128
THETA = 10000
F32 = jnp.float32
BF = jnp.bfloat16
GROUP = 4
SLOTS = 12


def normed(x, gain):
    wide = x.astype(jnp.float32)
    scale = lax.rsqrt(jnp.mean(wide * wide, -1, keepdims=True) + 1e-6)
    return (wide * scale * gain.astype(jnp.float32)).astype(jnp.bfloat16)


def turned(t, place, theta):
    half = t.shape[-1] // 2
    angle = place.astype(jnp.float32)[:, None] * theta ** (-jnp.arange(half, dtype=jnp.float32) / half)
    cos, sin = jnp.cos(angle)[:, None], jnp.sin(angle)[:, None]
    a, b = t[..., :half].astype(jnp.float32), t[..., half:].astype(jnp.float32)
    return jnp.concatenate([a * cos - b * sin, b * cos + a * sin], -1).astype(jnp.bfloat16)


def matmul(a, w):
    return jnp.dot(a, w, preferred_element_type=jnp.float32).astype(jnp.bfloat16)


def scores_of(q, k_ref):
    rows = k_ref.shape[0] // 2
    both = jnp.concatenate([k_ref[0:rows, :], k_ref[rows : 2 * rows, :]], axis=1)
    return lax.dot_general(q, both, (((1,), (1,)), ((), ())), preferred_element_type=F32)


def weights_of(s):
    row, lane = lax.broadcasted_iota(jnp.int32, s.shape, 0), lax.broadcasted_iota(jnp.int32, s.shape, 1)
    s = jnp.where((row & 3) == (lane & 3), s * HEAD**-0.5, -jnp.inf)
    top = jnp.max(s, axis=1, keepdims=True)
    top = jnp.maximum(top, jnp.concatenate([top[4:], top[:4]], 0))
    e = jnp.exp(s - top)
    total = jnp.sum(e, axis=1, keepdims=True)
    total = total + jnp.concatenate([total[4:], total[:4]], 0)
    return (e * (1.0 / total)).astype(BF)


def mixed(p, v_ref):
    rows = v_ref.shape[0] // 2
    both = jnp.concatenate([v_ref[0:rows, :], v_ref[rows : 2 * rows, :]], axis=1)
    o = jnp.dot(p, both, preferred_element_type=F32)
    return o[0:4, 0:HEAD] + o[4:8, HEAD : 2 * HEAD]


def attention_kernel(q_ref, k_hbm, v_hbm, o_ref, kb, vb, sb, k_sem, v_sem):
    batch = k_hbm.shape[0]
    steps = batch // GROUP

    def k_copy(b):
        slot = lax.rem(b, SLOTS)
        return pltpu.make_async_copy(k_hbm.at[b], kb.at[slot], k_sem.at[slot])

    def v_copy(b):
        slot = lax.rem(b, SLOTS)
        return pltpu.make_async_copy(v_hbm.at[b], vb.at[slot], v_sem.at[slot])

    def first(b, carry):
        k_copy(b).start()
        v_copy(b).start()
        return carry

    lax.fori_loop(0, SLOTS, first, 0)

    def wait(copy, t):
        for j in range(GROUP):
            copy(t * GROUP + j).wait()

    def refill(copy, t):
        for j in range(GROUP):
            b = t * GROUP + j

            @pl.when(b + SLOTS < batch)
            def _():
                copy(b + SLOTS).start()

    def score(t):
        for j in range(GROUP):
            b = t * GROUP + j
            sb[lax.rem(t, 2), j] = scores_of(q_ref[b].astype(BF), kb.at[lax.rem(b, SLOTS)])

    def mix(t):
        ps = [weights_of(sb[lax.rem(t, 2), j]) for j in range(GROUP)]
        for j in range(GROUP):
            b = t * GROUP + j
            o_ref[b] = mixed(ps[j], vb.at[lax.rem(b, SLOTS)])

    wait(k_copy, 0)
    score(0)

    def body(t, carry):
        wait(v_copy, t)
        wait(k_copy, t + 1)
        refill(k_copy, t)
        score(t + 1)
        mix(t)
        refill(v_copy, t)
        return carry

    lax.fori_loop(0, steps - 1, body, 0)
    wait(v_copy, steps - 1)
    mix(steps - 1)


def attention(q, k, v):
    batch, rows = k.shape[:2]
    q = q.astype(F32)
    none = jnp.zeros_like(q)
    q = jnp.concatenate([jnp.concatenate([q, none], 2), jnp.concatenate([none, q], 2)], 1)
    return pl.pallas_call(
        attention_kernel,
        out_shape=jax.ShapeDtypeStruct((batch, 4, HEAD), F32),
        in_specs=[pl.BlockSpec(memory_space=pltpu.VMEM)] + [pl.BlockSpec(memory_space=pl.ANY)] * 2,
        out_specs=pl.BlockSpec(memory_space=pltpu.VMEM),
        scratch_shapes=[
            pltpu.VMEM((SLOTS, rows, HEAD), BF),
            pltpu.VMEM((SLOTS, rows, HEAD), BF),
            pltpu.VMEM((2, GROUP, 8, rows // 2), F32),
            pltpu.SemaphoreType.DMA((SLOTS,)),
            pltpu.SemaphoreType.DMA((SLOTS,)),
        ],
        compiler_params=pltpu.CompilerParams(vmem_limit_bytes=56 * 2**20),
        name="attention",
    )(q, k, v)


CHIPS = 8


def added_kernel(term, t_ref, out_ref, near, mine, parts, whole, near_sem, part_sem, back_sem, pass_sem):
    me = lax.axis_index("tp")
    core, chip = lax.rem(me, 2), me // 2
    twin = chip * 2 + (1 - core)
    width = term.shape[1] // (2 * CHIPS)
    half = width * CHIPS

    def peer(d):
        return lax.rem(chip + d, CHIPS)

    def columns(o, w):
        return pl.ds(pl.multiple_of(o * w, w), w)

    def copy(src, dst, sems, i, device):
        return pltpu.make_async_remote_copy(
            src_ref=src, dst_ref=dst, send_sem=sems.at[0, i], recv_sem=sems.at[1, i],
            device_id={"tp": device}, device_id_type=pl.DeviceIdType.MESH,
        )

    barrier = pltpu.get_barrier_semaphore()
    pl.semaphore_signal(barrier, inc=1, device_id={"tp": twin}, device_id_type=pl.DeviceIdType.MESH)
    for d in range(1, CHIPS):
        pl.semaphore_signal(barrier, inc=1, device_id={"tp": peer(d) * 2 + core}, device_id_type=pl.DeviceIdType.MESH)
    pl.semaphore_wait(barrier, CHIPS)

    over = copy(term.at[:, columns(1 - core, half)], near, near_sem, 0, twin)
    over.start()
    over.wait()
    mine[...] = (term[:, columns(core, half)].astype(F32) + near[...].astype(F32)).astype(BF)
    out = []
    for d in range(1, CHIPS):
        c = copy(mine.at[:, columns(peer(d), width)], parts.at[d], part_sem, d, peer(d) * 2 + core)
        c.start()
        out.append(c)
    own = core * CHIPS + chip
    total = term[:, columns(own, width)].astype(F32) + near[:, columns(chip, width)].astype(F32)
    for c in out:
        c.wait()
    for d in range(1, CHIPS):
        total = total + parts[d].astype(F32)
    whole[:, columns(own, width)] = (t_ref[:, columns(own, width)].astype(F32) + total).astype(BF)

    passed = copy(whole.at[:, columns(own, width)], whole.at[:, columns(own, width)], pass_sem, 0, twin)
    back = []
    for d in range(1, CHIPS):
        c = copy(whole.at[:, columns(own, width)], whole.at[:, columns(own, width)], back_sem, d, peer(d) * 2 + core)
        c.start()
        back.append(c)
    passed.start()
    on = [passed]
    for d in range(1, CHIPS):
        back[d - 1].wait_recv()
        block = columns(core * CHIPS + lax.rem(chip + CHIPS - d, CHIPS), width)
        c = copy(whole.at[:, block], whole.at[:, block], pass_sem, d, twin)
        c.start()
        on.append(c)
    for c in back:
        c.wait_send()
    for c in on:
        c.wait()
    out_ref[...] = whole[...]


def added(t, term, number):
    rows, d = t.shape
    width = d // (2 * CHIPS)
    return pl.pallas_call(
        added_kernel,
        out_shape=jax.ShapeDtypeStruct((rows, d), BF),
        in_specs=[pl.BlockSpec(memory_space=pltpu.VMEM)] * 2,
        out_specs=pl.BlockSpec(memory_space=pltpu.VMEM),
        scratch_shapes=[
            pltpu.VMEM((rows, d // 2), BF),
            pltpu.VMEM((rows, d // 2), BF),
            pltpu.VMEM((CHIPS, rows, width), BF),
            pltpu.VMEM((rows, d), BF),
            pltpu.SemaphoreType.DMA((2, 1)),
            pltpu.SemaphoreType.DMA((2, CHIPS)),
            pltpu.SemaphoreType.DMA((2, CHIPS)),
            pltpu.SemaphoreType.DMA((2, CHIPS)),
        ],
        compiler_params=pltpu.CompilerParams(collective_id=number, has_side_effects=True, vmem_limit_bytes=16 * 2**20),
        name=f"added_{number}",
    )(term.astype(BF), t)


def hidden_of(b, w_gate, w_up):
    gate = jnp.dot(b, w_gate, preferred_element_type=jnp.float32)
    up = jnp.dot(b, w_up, preferred_element_type=jnp.float32)
    return (jax.nn.silu(gate) * up).astype(jnp.bfloat16)


def solution(mesh):
    def step(x, k_cache, v_cache, gain_a, wq, wo, gain_m, w_gate, w_up, w_down):
        batch, cache, heads = k_cache.shape[:3]
        place = jnp.full((batch,), cache - 1)
        q = turned(matmul(normed(x, gain_a), wq).reshape(batch, heads, HEAD), place, THETA)
        seen = attention(q, k_cache.reshape(batch, cache * heads, HEAD), v_cache.reshape(batch, cache * heads, HEAD))
        seen = seen.astype(BF).reshape(batch, heads * HEAD)
        h = added(x, jnp.dot(seen, wo, preferred_element_type=jnp.float32), 0)
        hidden = hidden_of(normed(h, gain_m), w_gate, w_up)
        return added(h, jnp.dot(hidden, w_down, preferred_element_type=jnp.float32), 1)

    states, cache, columns, rows_of = P("dp", None), P("dp", None, "tp", None), P(None, "tp"), P("tp", None)
    return jax.shard_map(
        step,
        mesh=mesh,
        in_specs=(states, cache, cache, P(None), columns, rows_of, P(None), columns, columns, rows_of),
        out_specs=states,
        check_vma=False,
    )
```

```python
import jax
import jax.numpy as jnp
from jax import lax
from jax.experimental import pallas as pl
from jax.experimental.pallas import tpu as pltpu
from jax.sharding import PartitionSpec as P

HEAD = 128
THETA = 10000
F32 = jnp.float32
BF = jnp.bfloat16
GROUP = 4
SLOTS = 12


def normed(x, gain):
    wide = x.astype(jnp.float32)
    scale = lax.rsqrt(jnp.mean(wide * wide, -1, keepdims=True) + 1e-6)
    return (wide * scale * gain.astype(jnp.float32)).astype(jnp.bfloat16)


def turned(t, place, theta):
    half = t.shape[-1] // 2
    angle = place.astype(jnp.float32)[:, None] * theta ** (-jnp.arange(half, dtype=jnp.float32) / half)
    cos, sin = jnp.cos(angle)[:, None], jnp.sin(angle)[:, None]
    a, b = t[..., :half].astype(jnp.float32), t[..., half:].astype(jnp.float32)
    return jnp.concatenate([a * cos - b * sin, b * cos + a * sin], -1).astype(jnp.bfloat16)


def matmul(a, w):
    return jnp.dot(a, w, preferred_element_type=jnp.float32).astype(jnp.bfloat16)


def scores_of(q, k_ref):
    rows = k_ref.shape[0] // 2
    both = jnp.concatenate([k_ref[0:rows, :], k_ref[rows : 2 * rows, :]], axis=1)
    return lax.dot_general(q, both, (((1,), (1,)), ((), ())), preferred_element_type=F32)


def weights_of(s):
    row, lane = lax.broadcasted_iota(jnp.int32, s.shape, 0), lax.broadcasted_iota(jnp.int32, s.shape, 1)
    s = jnp.where((row & 3) == (lane & 3), s * HEAD**-0.5, -jnp.inf)
    top = jnp.max(s, axis=1, keepdims=True)
    top = jnp.maximum(top, jnp.concatenate([top[4:], top[:4]], 0))
    e = jnp.exp(s - top)
    total = jnp.sum(e, axis=1, keepdims=True)
    total = total + jnp.concatenate([total[4:], total[:4]], 0)
    return (e * (1.0 / total)).astype(BF)


def mixed(p, v_ref):
    rows = v_ref.shape[0] // 2
    both = jnp.concatenate([v_ref[0:rows, :], v_ref[rows : 2 * rows, :]], axis=1)
    o = jnp.dot(p, both, preferred_element_type=F32)
    return o[0:4, 0:HEAD] + o[4:8, HEAD : 2 * HEAD]


def attention_kernel(q_ref, k_hbm, v_hbm, o_ref, kb, vb, sb, k_sem, v_sem):
    batch = k_hbm.shape[0]
    steps = batch // GROUP

    def k_copy(b):
        slot = lax.rem(b, SLOTS)
        return pltpu.make_async_copy(k_hbm.at[b], kb.at[slot], k_sem.at[slot])

    def v_copy(b):
        slot = lax.rem(b, SLOTS)
        return pltpu.make_async_copy(v_hbm.at[b], vb.at[slot], v_sem.at[slot])

    def first(b, carry):
        k_copy(b).start()
        v_copy(b).start()
        return carry

    lax.fori_loop(0, SLOTS, first, 0)

    def wait(copy, t):
        for j in range(GROUP):
            copy(t * GROUP + j).wait()

    def refill(copy, t):
        for j in range(GROUP):
            b = t * GROUP + j

            @pl.when(b + SLOTS < batch)
            def _():
                copy(b + SLOTS).start()

    def score(t):
        for j in range(GROUP):
            b = t * GROUP + j
            sb[lax.rem(t, 2), j] = scores_of(q_ref[b].astype(BF), kb.at[lax.rem(b, SLOTS)])

    def mix(t):
        ps = [weights_of(sb[lax.rem(t, 2), j]) for j in range(GROUP)]
        for j in range(GROUP):
            b = t * GROUP + j
            o_ref[b] = mixed(ps[j], vb.at[lax.rem(b, SLOTS)])

    wait(k_copy, 0)
    score(0)

    def body(t, carry):
        wait(v_copy, t)
        wait(k_copy, t + 1)
        refill(k_copy, t)
        score(t + 1)
        mix(t)
        refill(v_copy, t)
        return carry

    lax.fori_loop(0, steps - 1, body, 0)
    wait(v_copy, steps - 1)
    mix(steps - 1)


def attention(q, k, v):
    batch, rows = k.shape[:2]
    q = q.astype(F32)
    none = jnp.zeros_like(q)
    q = jnp.concatenate([jnp.concatenate([q, none], 2), jnp.concatenate([none, q], 2)], 1)
    return pl.pallas_call(
        attention_kernel,
        out_shape=jax.ShapeDtypeStruct((batch, 4, HEAD), F32),
        in_specs=[pl.BlockSpec(memory_space=pltpu.VMEM)] + [pl.BlockSpec(memory_space=pl.ANY)] * 2,
        out_specs=pl.BlockSpec(memory_space=pltpu.VMEM),
        scratch_shapes=[
            pltpu.VMEM((SLOTS, rows, HEAD), BF),
            pltpu.VMEM((SLOTS, rows, HEAD), BF),
            pltpu.VMEM((2, GROUP, 8, rows // 2), F32),
            pltpu.SemaphoreType.DMA((SLOTS,)),
            pltpu.SemaphoreType.DMA((SLOTS,)),
        ],
        compiler_params=pltpu.CompilerParams(vmem_limit_bytes=56 * 2**20),
        name="attention",
    )(q, k, v)


CHIPS = 8


def exchanged(term, t_ref, near, mine, parts, whole, near_sem, part_sem, back_sem, pass_sem):
    me = lax.axis_index("tp")
    core, chip = lax.rem(me, 2), me // 2
    twin = chip * 2 + (1 - core)
    width = term.shape[1] // (2 * CHIPS)
    half = width * CHIPS

    def peer(d):
        return lax.rem(chip + d, CHIPS)

    def columns(o, w):
        return pl.ds(pl.multiple_of(o * w, w), w)

    def copy(src, dst, sems, i, device):
        return pltpu.make_async_remote_copy(
            src_ref=src, dst_ref=dst, send_sem=sems.at[0, i], recv_sem=sems.at[1, i],
            device_id={"tp": device}, device_id_type=pl.DeviceIdType.MESH,
        )

    barrier = pltpu.get_barrier_semaphore()
    pl.semaphore_signal(barrier, inc=1, device_id={"tp": twin}, device_id_type=pl.DeviceIdType.MESH)
    for d in range(1, CHIPS):
        pl.semaphore_signal(barrier, inc=1, device_id={"tp": peer(d) * 2 + core}, device_id_type=pl.DeviceIdType.MESH)
    pl.semaphore_wait(barrier, CHIPS)

    over = copy(term.at[:, columns(1 - core, half)], near, near_sem, 0, twin)
    over.start()
    over.wait()
    mine[...] = (term[:, columns(core, half)].astype(F32) + near[...].astype(F32)).astype(BF)
    out = []
    for d in range(1, CHIPS):
        c = copy(mine.at[:, columns(peer(d), width)], parts.at[d], part_sem, d, peer(d) * 2 + core)
        c.start()
        out.append(c)
    own = core * CHIPS + chip
    total = term[:, columns(own, width)].astype(F32) + near[:, columns(chip, width)].astype(F32)
    for c in out:
        c.wait()
    for d in range(1, CHIPS):
        total = total + parts[d].astype(F32)
    whole[:, columns(own, width)] = (t_ref[:, columns(own, width)].astype(F32) + total).astype(BF)

    passed = copy(whole.at[:, columns(own, width)], whole.at[:, columns(own, width)], pass_sem, 0, twin)
    back = []
    for d in range(1, CHIPS):
        c = copy(whole.at[:, columns(own, width)], whole.at[:, columns(own, width)], back_sem, d, peer(d) * 2 + core)
        c.start()
        back.append(c)
    passed.start()
    on = [passed]
    for d in range(1, CHIPS):
        back[d - 1].wait_recv()
        block = columns(core * CHIPS + lax.rem(chip + CHIPS - d, CHIPS), width)
        c = copy(whole.at[:, block], whole.at[:, block], pass_sem, d, twin)
        c.start()
        on.append(c)
    for c in back:
        c.wait_send()
    for c in on:
        c.wait()


def added_kernel(term, t_ref, out_ref, near, mine, parts, whole, *sems):
    exchanged(term, t_ref, near, mine, parts, whole, *sems)
    out_ref[...] = whole[...]


def scratch_of(rows, d):
    width = d // (2 * CHIPS)
    return [
        pltpu.VMEM((rows, d // 2), BF),
        pltpu.VMEM((rows, d // 2), BF),
        pltpu.VMEM((CHIPS, rows, width), BF),
        pltpu.VMEM((rows, d), BF),
        pltpu.SemaphoreType.DMA((2, 1)),
        pltpu.SemaphoreType.DMA((2, CHIPS)),
        pltpu.SemaphoreType.DMA((2, CHIPS)),
        pltpu.SemaphoreType.DMA((2, CHIPS)),
    ]


def added(t, term, number):
    rows, d = t.shape
    return pl.pallas_call(
        added_kernel,
        out_shape=jax.ShapeDtypeStruct((rows, d), BF),
        in_specs=[pl.BlockSpec(memory_space=pltpu.VMEM)] * 2,
        out_specs=pl.BlockSpec(memory_space=pltpu.VMEM),
        scratch_shapes=scratch_of(rows, d),
        compiler_params=pltpu.CompilerParams(collective_id=number, has_side_effects=True, vmem_limit_bytes=16 * 2**20),
        name=f"added_{number}",
    )(term.astype(BF), t)


DEPTH = 1024
PANEL = 1024
AHEAD = 4
PANELS = 5


def second_kernel(term, t_ref, gain_ref, gate_hbm, up_hbm, down_hbm, h_ref, out_ref, gates, ups, downs, gate, up, w_sem, d_sem, near, mine, parts, whole, *sems):
    d = t_ref.shape[1]
    steps, panels = d // DEPTH, d // PANEL

    def gate_copy(i):
        slot = lax.rem(i, AHEAD)
        return pltpu.make_async_copy(gate_hbm.at[pl.ds(pl.multiple_of(i * DEPTH, DEPTH), DEPTH), :], gates.at[slot], w_sem.at[0, slot])

    def up_copy(i):
        slot = lax.rem(i, AHEAD)
        return pltpu.make_async_copy(up_hbm.at[pl.ds(pl.multiple_of(i * DEPTH, DEPTH), DEPTH), :], ups.at[slot], w_sem.at[1, slot])

    def down_copy(i):
        slot = lax.rem(i, PANELS)
        return pltpu.make_async_copy(down_hbm.at[:, pl.ds(pl.multiple_of(i * PANEL, PANEL), PANEL)], downs.at[slot], d_sem.at[slot])

    def first(i, carry):
        gate_copy(i).start()
        up_copy(i).start()
        return carry

    def first_down(i, carry):
        down_copy(i).start()
        return carry

    lax.fori_loop(0, AHEAD, first, 0)
    lax.fori_loop(0, PANELS, first_down, 0)
    exchanged(term, t_ref, near, mine, parts, whole, *sems)

    def piece(i):
        return pl.ds(pl.multiple_of(i * DEPTH, DEPTH), DEPTH)

    def squares(i, total):
        wide = whole[:, piece(i)].astype(F32)
        h_ref[:, piece(i)] = whole[:, piece(i)]
        return total + jnp.sum(wide * wide, -1, keepdims=True)

    square = lax.fori_loop(0, steps, squares, jnp.zeros((t_ref.shape[0], 1), F32))
    scale = lax.rsqrt(square / d + 1e-6)
    gate[...] = jnp.zeros_like(gate)
    up[...] = jnp.zeros_like(up)

    def body(i, carry):
        slot = lax.rem(i, AHEAD)
        b = (whole[:, piece(i)].astype(F32) * scale * gain_ref[:, piece(i)].astype(F32)).astype(BF)
        gate_copy(i).wait()
        up_copy(i).wait()
        gate[...] += jnp.dot(b, gates[slot], preferred_element_type=F32)
        up[...] += jnp.dot(b, ups[slot], preferred_element_type=F32)

        @pl.when(i + AHEAD < steps)
        def _():
            gate_copy(i + AHEAD).start()
            up_copy(i + AHEAD).start()

        return carry

    lax.fori_loop(0, steps, body, 0)
    hidden = (jax.nn.silu(gate[...]) * up[...]).astype(BF)

    def panel(i, carry):
        down_copy(i).wait()
        out_ref[:, pl.ds(pl.multiple_of(i * PANEL, PANEL), PANEL)] = jnp.dot(hidden, downs[lax.rem(i, PANELS)], preferred_element_type=F32).astype(BF)

        @pl.when(i + PANELS < panels)
        def _():
            down_copy(i + PANELS).start()

        return carry

    lax.fori_loop(0, panels, panel, 0)


def second(t, term, gain, w_gate, w_up, w_down):
    rows, d = t.shape
    units = w_gate.shape[1]
    return pl.pallas_call(
        second_kernel,
        out_shape=[jax.ShapeDtypeStruct((rows, d), BF)] * 2,
        in_specs=[pl.BlockSpec(memory_space=pltpu.VMEM)] * 3 + [pl.BlockSpec(memory_space=pl.ANY)] * 3,
        out_specs=[pl.BlockSpec(memory_space=pltpu.VMEM)] * 2,
        scratch_shapes=[
            pltpu.VMEM((AHEAD, DEPTH, units), BF),
            pltpu.VMEM((AHEAD, DEPTH, units), BF),
            pltpu.VMEM((PANELS, units, PANEL), BF),
            pltpu.VMEM((rows, units), F32),
            pltpu.VMEM((rows, units), F32),
            pltpu.SemaphoreType.DMA((2, AHEAD)),
            pltpu.SemaphoreType.DMA((PANELS,)),
        ]
        + scratch_of(rows, d),
        compiler_params=pltpu.CompilerParams(collective_id=0, has_side_effects=True, vmem_limit_bytes=58 * 2**20),
        name="second",
    )(term.astype(BF), t, gain.reshape(1, d), w_gate, w_up, w_down)


def solution(mesh):
    def step(x, k_cache, v_cache, gain_a, wq, wo, gain_m, w_gate, w_up, w_down):
        batch, cache, heads = k_cache.shape[:3]
        place = jnp.full((batch,), cache - 1)
        q = turned(matmul(normed(x, gain_a), wq).reshape(batch, heads, HEAD), place, THETA)
        seen = attention(q, k_cache.reshape(batch, cache * heads, HEAD), v_cache.reshape(batch, cache * heads, HEAD))
        seen = seen.astype(BF).reshape(batch, heads * HEAD)
        h, term = second(x, jnp.dot(seen, wo, preferred_element_type=jnp.float32), gain_m, w_gate, w_up, w_down)
        return added(h, term, 1)

    states, cache, columns, rows_of = P("dp", None), P("dp", None, "tp", None), P(None, "tp"), P("tp", None)
    return jax.shard_map(
        step,
        mesh=mesh,
        in_specs=(states, cache, cache, P(None), columns, rows_of, P(None), columns, columns, rows_of),
        out_specs=states,
        check_vma=False,
    )
```
